256 devices in a mesh: first: 16 (over y, x), second: 16 (over z, core).
Axes of the slice: x: 4, y: 4, z: 8, core: 2. Of those that a mesh axis runs over, the one named last changes fastest.
Arguments:
- pair_state: bfloat16 [768, 768, 128], P('first', 'second'), may hold values from -6 to 6
- in_gain: float32 [128], replicated, may hold values from 0.25 to 1.75
- left_weight: bfloat16 [128, 128], replicated, may hold values from -0.5 to 0.5
- right_weight: bfloat16 [128, 128], replicated, may hold values from -0.5 to 0.5
- mid_gain: float32 [128], replicated, may hold values from 0.25 to 1.75
- out_weight: bfloat16 [128, 128], replicated, may hold values from -0.5 to 0.5
- out_gate: bfloat16 [128, 128], replicated, may hold values from -0.5 to 0.5
Outputs:
- triangle_out: bfloat16 [768, 768, 128], P('first', 'second')
The draws below stay inside these ranges and needn't reach their ends.
All inputs are finite; a program needn't handle non-finite values.
Results may differ from the reference program's by a relative error of at most 0.015.
Values may be sent and summed in bfloat16 or wider, within the bound.
A program may use at most 64 MiB of HBM per device.

```python
import jax
import jax.numpy as jnp
from jax import lax

RESIDUES = 768
PAIR_WIDTH = 128
MIX_WIDTH = 128


def shard_levels(own_key, extent, cuts, smallest, largest):
    def one(axis_at, parts):
        draws = jax.random.uniform(jax.random.fold_in(jax.random.fold_in(own_key, 6), axis_at), (parts,), jnp.float32, smallest / len(cuts), largest / len(cuts))
        return jnp.repeat(jnp.exp(draws), extent[axis_at] // parts).reshape((-1,) + (1,) * (len(extent) - axis_at - 1))

    factor_of = one(*cuts[0])
    for cut in cuts[1:]:
        factor_of = factor_of * one(*cut)
    return factor_of


def scatter_about(key, extent, scale, bound, split=(), kind=jnp.bfloat16):
    gain = shard_levels(key, extent, split, -0.22, 0.18) if split else 1.0
    values = jax.random.normal(key, extent, jnp.float32) * scale * gain
    return jnp.minimum(jnp.maximum(values, -bound), bound).astype(kind)


def setup_inputs(seed: int = 0) -> dict:
    arg_keys = jax.random.split(jax.random.key(seed), 8)
    return {
        "pair_state": scatter_about(arg_keys[0], (RESIDUES, RESIDUES, PAIR_WIDTH), 1.0, 6.0, ((0, 16), (1, 16))),
        "in_gain": jnp.clip(1.0 + 0.15 * jax.random.normal(arg_keys[1], (PAIR_WIDTH,), jnp.float32), 0.25, 1.75),
        "left_weight": scatter_about(arg_keys[2], (PAIR_WIDTH, MIX_WIDTH), PAIR_WIDTH ** -0.5, 0.5),
        "right_weight": scatter_about(arg_keys[3], (PAIR_WIDTH, MIX_WIDTH), PAIR_WIDTH ** -0.5, 0.5),
        "mid_gain": jnp.clip(1.0 + 0.15 * jax.random.normal(arg_keys[4], (MIX_WIDTH,), jnp.float32), 0.25, 1.75),
        "out_weight": scatter_about(arg_keys[5], (MIX_WIDTH, PAIR_WIDTH), MIX_WIDTH ** -0.5, 0.5),
        "out_gate": scatter_about(arg_keys[6], (PAIR_WIDTH, PAIR_WIDTH), PAIR_WIDTH ** -0.5, 0.5),
    }


def unit_channels(values, channel_gain):
    centred = values - lax.optimization_barrier(jnp.mean(values, axis=-1, keepdims=True))
    return centred * lax.rsqrt(lax.optimization_barrier(jnp.mean(centred * centred, axis=-1, keepdims=True)) + 1e-05) * channel_gain

def make_factors(pair_in, in_gain, left_weight, right_weight):
    ready = unit_channels(pair_in.astype(jnp.float32), in_gain).astype(jnp.bfloat16)
    ready = lax.optimization_barrier(ready)
    left = jnp.einsum('ijc,cd->ijd', ready.astype(jnp.float32), left_weight.astype(jnp.float32))
    right = jnp.einsum('ijc,cd->ijd', ready.astype(jnp.float32), right_weight.astype(jnp.float32))
    return (ready, left.astype(jnp.bfloat16), right.astype(jnp.bfloat16))

def finish_pair(mixed, ready, mid_gain, out_weight, out_gate):
    scaled = unit_channels(mixed.astype(jnp.float32), mid_gain).astype(jnp.bfloat16)
    scaled = lax.optimization_barrier(scaled)
    gate = jax.nn.sigmoid(jnp.einsum('ijc,cd->ijd', ready.astype(jnp.float32), out_gate.astype(jnp.float32)))
    return (jnp.einsum('ijd,dc->ijc', scaled.astype(jnp.float32), out_weight.astype(jnp.float32)) * gate).astype(jnp.bfloat16)

def reference(pair_state, in_gain, left_weight, right_weight, mid_gain, out_weight, out_gate):
    ready, left, right = make_factors(pair_state, in_gain, left_weight, right_weight)
    left, right = lax.optimization_barrier((left, right))

    def one_channel(pair_of):
        return (jnp.dot(pair_of[0], pair_of[1].T, preferred_element_type=jnp.float32) * RESIDUES ** (-0.5)).astype(jnp.bfloat16)
    mixed = jnp.moveaxis(lax.map(one_channel, (jnp.moveaxis(left, -1, 0), jnp.moveaxis(right, -1, 0))), 0, -1)
    mixed = lax.optimization_barrier(mixed)
    return finish_pair(mixed, ready, mid_gain, out_weight, out_gate)
```

```python
import functools

import jax
import jax.numpy as jnp
from jax import lax
from jax.experimental import pallas as pl
from jax.experimental.pallas import tpu as pltpu
from jax.sharding import PartitionSpec as P

MESH = pl.DeviceIdType.MESH
F32, BF16 = jnp.float32, jnp.bfloat16
VMEM = pl.BlockSpec(memory_space=pltpu.VMEM)


def norm(values, gain, axis):
    centred = values - jnp.mean(values, axis=axis, keepdims=True)
    scale = lax.rsqrt(jnp.mean(centred * centred, axis=axis, keepdims=True) + 1e-05)
    return centred * scale * gain


def place():
    a, b = lax.axis_index("first"), lax.axis_index("second")
    return a, b, a // 8, a * 8 + b // 2, lax.rem(b, 2)


def chip(c, core):
    return (c // 8, lax.rem(c, 8) * 2 + core)


def factor_rows(x_ref, gain_ref, wl_ref, wr_ref, rows_ref, msg_ref):
    weights = jnp.concatenate([wr_ref[...].astype(F32).T, wl_ref[...].astype(F32).T], axis=0)
    weights = weights.astype(BF16)
    gain = gain_ref[...]

    def tile(r, _):
        k1, i1 = r // 6, lax.rem(r, 6)
        block = x_ref[pl.ds(i1 * 8, 8), pl.ds(pl.multiple_of(k1 * 16, 16), 16), :]
        ready = norm(block.astype(F32).reshape(128, 128), gain, 1).astype(BF16)
        made = lax.dot_general(
            weights, ready, (((1,), (1,)), ((), ())), preferred_element_type=F32
        )
        rows_ref[pl.ds(r, 256, stride=24), :] = made
        return 0

    lax.fori_loop(0, 18, tile, 0)

    def pack(d, _):
        for e in range(8):
            at = d * 8 + e
            msg_ref[at] = rows_ref[pl.ds(pl.multiple_of(at * 24, 8), 24), :][:18].astype(BF16)
        return 0

    lax.fori_loop(0, 32, pack, 0)


def factor_kernel(x_ref, gain_ref, wl_ref, wr_ref, l_ref, r_ref, rows_ref, msg_ref, sems):
    a, b, half, mine, core = place()
    barrier = pltpu.get_barrier_semaphore()

    def greet(c, _):
        pl.semaphore_signal(
            barrier, inc=1, device_id=(c // 16 + 8 * core, lax.rem(c, 16)), device_id_type=MESH
        )
        return 0

    lax.fori_loop(0, 128, greet, 0)
    pl.semaphore_signal(barrier, inc=1, device_id=(a, b + 1 - 2 * core), device_id_type=MESH)
    factor_rows(x_ref, gain_ref, wl_ref, wr_ref, rows_ref, msg_ref)
    pl.semaphore_wait(barrier, 129)

    slot = lax.rem(a, 8) * 16 + b
    own = half == core

    def send(which, dest_ref, base, send_sem, recv_sem):
        def one(t, _):
            c = lax.rem(mine + t, 128)

            @pl.when(jnp.logical_or(t > 0, jnp.logical_not(own)))
            def _():
                pltpu.make_async_remote_copy(
                    src_ref=msg_ref.at[which * 128 + c],
                    dst_ref=dest_ref.at[base + slot],
                    send_sem=send_sem,
                    recv_sem=recv_sem,
                    device_id=chip(c, half),
                    device_id_type=MESH,
                ).start()

            return 0

        lax.fori_loop(0, 128, one, 0)

        @pl.when(own)
        def _():
            dest_ref[base + slot] = msg_ref[which * 128 + mine]

    def settle(ref, sem):
        @pl.when(own)
        def _():
            view = ref.at[pl.ds(0, 127)]
            pltpu.make_async_copy(view, view, sem).wait()

        @pl.when(jnp.logical_not(own))
        def _():
            view = ref.at[pl.ds(0, 128)]
            pltpu.make_async_copy(view, view, sem).wait()

    send(0, r_ref, half * 128, sems.at[0], sems.at[1])
    send(1, l_ref, 0, sems.at[2], sems.at[3])
    settle(r_ref, sems.at[1])
    swap = pltpu.make_async_remote_copy(
        src_ref=r_ref.at[pl.ds(core * 128, 128)],
        dst_ref=r_ref.at[pl.ds(core * 128, 128)],
        send_sem=sems.at[4],
        recv_sem=sems.at[5],
        device_id=(a, b + 1 - 2 * core),
        device_id_type=MESH,
    )
    swap.start()
    settle(l_ref, sems.at[3])
    swap.wait()
    settle(msg_ref, sems.at[0])
    settle(msg_ref, sems.at[2])


def product_rows(l_ref, r_ref, c_ref, pad_ref, rk_ref, lf_ref, lb_ref, z_ref, g_ref):
    lane = lax.broadcasted_iota(jnp.int32, (64, 128), 1)

    def quarter(h, _):
        groups = []
        for bb in range(8):
            b = h * 8 + bb
            for ja in range(16):
                pad_ref[ja, 0:18, :] = r_ref[ja * 16 + b].astype(F32)
            for k1 in range(3):
                block = pad_ref[:, k1 * 6 : k1 * 6 + 8, :].reshape(128, 128).T
                at = pl.multiple_of(b * 48 + k1 * 16, 16)
                for j0 in range(8):
                    rk_ref[pl.ds(at, 16), j0 * 128 : (j0 + 1) * 128] = block[
                        j0 * 16 : (j0 + 1) * 16
                    ].astype(BF16)
        for bb in range(8):
            b = h * 8 + bb
            for ia in range(8):
                pad_ref[ia, 0:18, :] = l_ref[ia * 16 + b].astype(F32)
            for k1 in range(3):
                groups.append(pad_ref[0:8, k1 * 6 : k1 * 6 + 8, :].reshape(64, 128))
            while len(groups) >= 8:
                blocks, groups = groups[:8], groups[8:]
                for bit in (1, 2, 4):
                    high = (lane // (16 * bit)) % 2 == 1
                    turned = list(blocks)
                    for n in range(8):
                        if n & bit:
                            continue
                        one, two = blocks[n], blocks[n + bit]
                        turned[n] = jnp.where(high, pltpu.roll(two, 16 * bit, 1), one)
                        turned[n + bit] = jnp.where(high, two, pltpu.roll(one, 128 - 16 * bit, 1))
                    blocks = turned
                tile = bb * 3 // 8
                for i0 in range(8):
                    for ia in range(8):
                        lf_ref[
                            pl.ds((h * 3 + tile) * 384 + ia * 48 + i0, 6, stride=8), :
                        ] = blocks[i0][ia * 8 : ia * 8 + 6]
        return 0

    lax.fori_loop(0, 2, quarter, 0)
    for tile in range(6):
        lb_ref[:, tile * 128 : (tile + 1) * 128] = lf_ref[
            tile * 384 : (tile + 1) * 384, :
        ].astype(BF16)
    for n in range(4):
        made = jnp.dot(
            lb_ref[...], rk_ref[:, n * 256 : (n + 1) * 256], preferred_element_type=F32
        )
        made = made * 768**-0.5
        z_ref[pl.ds(2 * n, 384, stride=8), :] = made[:, :128]
        z_ref[pl.ds(2 * n + 1, 384, stride=8), :] = made[:, 128:]

    def give(ia, _):
        for ih in range(3):
            at = pl.multiple_of((ia * 3 + ih) * 128, 128)
            block = z_ref[pl.ds(at, 128), :].T
            for jb in range(16):
                g_ref[jb, ih * 6 : ih * 6 + 6, :] = block[jb * 8 : jb * 8 + 6]
        for jb in range(16):
            c_ref[ia * 16 + jb] = g_ref[jb][:18].astype(BF16)
        return 0

    lax.fori_loop(0, 8, give, 0)


def return_kernel(c_ref, d_ref, sems):
    a, b, half, mine, core = place()
    barrier = pltpu.get_barrier_semaphore()

    def greet(c, _):
        pl.semaphore_signal(barrier, inc=1, device_id=chip(c, half), device_id_type=MESH)
        return 0

    lax.fori_loop(0, 128, greet, 0)
    pl.semaphore_wait(barrier, 128)
    own = half == core
    home = lax.rem(a, 8) * 16 + b

    def one(t, _):
        s = lax.rem(home + t, 128)

        @pl.when(jnp.logical_or(t > 0, jnp.logical_not(own)))
        def _():
            pltpu.make_async_remote_copy(
                src_ref=c_ref.at[s],
                dst_ref=d_ref.at[mine],
                send_sem=sems.at[0],
                recv_sem=sems.at[1],
                device_id=(core * 8 + s // 16, lax.rem(s, 16)),
                device_id_type=MESH,
            ).start()

        return 0

    lax.fori_loop(0, 128, one, 0)

    @pl.when(own)
    def _():
        d_ref[mine] = c_ref[home]

    for sem in (sems.at[0], sems.at[1]):

        @pl.when(own)
        def _():
            view = d_ref.at[pl.ds(0, 127)]
            pltpu.make_async_copy(view, view, sem).wait()

        @pl.when(jnp.logical_not(own))
        def _():
            view = d_ref.at[pl.ds(0, 128)]
            pltpu.make_async_copy(view, view, sem).wait()


def finish_kernel(
    d_ref, x_ref, in_gain_ref, mid_gain_ref, w_ref, wg_ref, out_ref, rows_ref
):
    def spread(d, _):
        for e in range(8):
            at = d * 8 + e
            rows_ref[pl.ds(pl.multiple_of(at * 24, 8), 18), :] = d_ref[at].astype(F32)
        return 0

    lax.fori_loop(0, 16, spread, 0)
    column = jnp.broadcast_to(mid_gain_ref[...], (128, 128)).T

    def tile(n, _):
        ih, jp = n // 3, lax.rem(n, 3)
        i_at, j_at = pl.ds(ih * 16, 16), pl.ds(pl.multiple_of(jp * 16, 16), 16)
        block = x_ref[i_at, j_at, :].astype(F32).reshape(256, 128)
        ready = norm(block, in_gain_ref[...], 1).astype(BF16)
        gate = jax.nn.sigmoid(jnp.dot(ready, wg_ref[...], preferred_element_type=F32))
        halves = []
        for e in range(2):
            mixed = rows_ref[pl.ds(ih * 6 + jp * 2 + e, 128, stride=24), :]
            scaled = norm(mixed, column, 0).T.astype(BF16)
            made = jnp.dot(scaled, w_ref[...], preferred_element_type=F32)
            halves.append(made.reshape(16, 8, 128))
        made = jnp.concatenate(halves, axis=1)
        out_ref[i_at, j_at, :] = (made * gate.reshape(16, 16, 128)).astype(BF16)
        return 0

    lax.fori_loop(0, 9, tile, 0)


def per_device(pair_state, in_gain, left_weight, right_weight, mid_gain, out_weight, out_gate):
    def shape(*s, t=BF16):
        return jax.ShapeDtypeStruct(s, t)

    in_row, mid_row = in_gain.reshape(1, 128), mid_gain.reshape(1, 128)
    left, right = pl.pallas_call(
        factor_kernel,
        name="factors",
        out_shape=(shape(128, 18, 128), shape(256, 18, 128)),
        in_specs=[VMEM] * 4,
        out_specs=(VMEM, VMEM),
        scratch_shapes=[
            pltpu.VMEM((256 * 24, 128), F32),
            pltpu.VMEM((256, 18, 128), BF16),
            pltpu.SemaphoreType.DMA((6,)),
        ],
        compiler_params=pltpu.CompilerParams(collective_id=1, has_side_effects=True),
    )(pair_state, in_row, left_weight, right_weight)
    products = pl.pallas_call(
        product_rows,
        name="products",
        out_shape=shape(128, 18, 128),
        in_specs=[VMEM] * 2,
        out_specs=VMEM,
        scratch_shapes=[
            pltpu.VMEM((16, 24, 128), F32),
            pltpu.VMEM((768, 1024), BF16),
            pltpu.VMEM((6 * 384, 128), F32),
            pltpu.VMEM((384, 768), BF16),
            pltpu.VMEM((3072, 128), F32),
            pltpu.VMEM((16, 24, 128), F32),
        ],
    )(left, right)
    mixed = pl.pallas_call(
        return_kernel,
        name="returns",
        out_shape=shape(128, 18, 128),
        in_specs=[VMEM],
        out_specs=VMEM,
        scratch_shapes=[pltpu.SemaphoreType.DMA((2,))],
        compiler_params=pltpu.CompilerParams(collective_id=2, has_side_effects=True),
    )(products)
    return pl.pallas_call(
        finish_kernel,
        name="finish",
        out_shape=shape(48, 48, 128),
        in_specs=[VMEM] * 6,
        out_specs=VMEM,
        scratch_shapes=[
            pltpu.VMEM((128 * 24, 128), F32),
        ],
    )(mixed, pair_state, in_row, mid_row, out_weight, out_gate)


def solution(mesh):
    in_specs = (P("first", "second", None), P(), P(), P(), P(), P(), P())
    out_specs = P("first", "second", None)
    return jax.shard_map(
        per_device, mesh=mesh, in_specs=in_specs, out_specs=out_specs, check_vma=False
    )
```

```python
import jax
import jax.numpy as jnp
from jax import lax
from jax.experimental import pallas as pl
from jax.experimental.pallas import tpu as pltpu
from jax.sharding import PartitionSpec as P

LOGICAL = pl.DeviceIdType.LOGICAL
F32, BF16 = jnp.float32, jnp.bfloat16
VMEM = pl.BlockSpec(memory_space=pltpu.VMEM)
NT = (((1,), (1,)), ((), ()))


def norm(values, gain, axis):
    centred = values - jnp.mean(values, axis=axis, keepdims=True)
    scale = lax.rsqrt(jnp.mean(centred * centred, axis=axis, keepdims=True) + 1e-05)
    return centred * scale * gain


def around(start, step, unroll=8):
    def at(t):
        c = start + t
        step(jnp.where(c >= 128, c - 128, c))

    def some(n, _):
        for e in range(unroll):
            at(n * unroll + e + 1)
        return 0

    lax.fori_loop(0, 127 // unroll, some, 0)
    for t in range(127 // unroll * unroll + 1, 128):
        at(jnp.int32(t))


def make_right(x_ref, gain_ref, w_ref, ready_ref, rows_ref, msg_ref):
    gain = gain_ref[...]
    weights = w_ref[...].astype(F32).T.astype(BF16)

    def tiles(k1, _):
        for i1 in range(6):
            block = x_ref[i1 * 8 : i1 * 8 + 8, pl.ds(pl.multiple_of(k1 * 16, 16), 16), :]
            ready = norm(block.astype(F32).reshape(128, 128), gain, 1).astype(BF16)
            ready_ref[k1 * 6 + i1] = ready
            made = lax.dot_general(weights, ready, NT, preferred_element_type=F32)
            rows_ref[pl.ds(k1 * 6 + i1, 128, stride=18), :] = made
        return 0

    lax.fori_loop(0, 3, tiles, 0)

    def pack(n, _):
        rows = rows_ref[pl.ds(pl.multiple_of(n * 288, 8), 288), :]
        msg_ref[pl.ds(n * 144, 144)] = rows.astype(BF16).reshape(144, 2, 128)
        return 0

    lax.fori_loop(0, 8, pack, 0)


def make_left(w_ref, ready_ref, rows_ref, msg_ref):
    weights = w_ref[...].astype(F32).T.astype(BF16)

    def tiles(k1, _):
        for i1 in range(6):
            made = lax.dot_general(
                weights, ready_ref[k1 * 6 + i1], NT, preferred_element_type=F32
            )
            at = (i1 // 2) * 768 + k1 * 2 + i1 % 2
            rows_ref[pl.ds(at, 128, stride=6), :] = made
        return 0

    lax.fori_loop(0, 3, tiles, 0)
    for ih in range(3):

        def pack(n, _):
            rows = rows_ref[pl.ds(pl.multiple_of(ih * 768 + n * 192, 8), 192), :]
            msg_ref[ih, pl.ds(n * 96, 96)] = rows.astype(BF16).reshape(96, 2, 128)
            return 0

        lax.fori_loop(0, 4, pack, 0)


def make_gate(w_ref, ready_ref, gate_ref):
    weights = w_ref[...]

    def tiles(k1, _):
        for i1 in range(6):
            made = jnp.dot(ready_ref[k1 * 6 + i1], weights, preferred_element_type=F32)
            gate = jax.nn.sigmoid(made).reshape(8, 16, 128)
            gate_ref[i1 * 8 : i1 * 8 + 8, pl.ds(pl.multiple_of(k1 * 16, 16), 16), :] = gate
        return 0

    lax.fori_loop(0, 3, tiles, 0)


def turn_right(in_ref, pad_ref, right_ref):
    def lines(n, _):
        for e in range(2):
            b = n * 2 + e
            pad_ref[e, 0:288, :] = in_ref[b].reshape(288, 128).astype(F32)
            for k1 in range(3):
                parts = [pad_ref[e, ja * 18 + k1 * 6 : ja * 18 + k1 * 6 + 8, :] for ja in range(16)]
                block = jnp.concatenate(parts, axis=0).T.astype(BF16)
                at = pl.multiple_of(b * 48 + k1 * 16, 16)
                for j0 in range(8):
                    right_ref[pl.ds(at, 16), j0 * 128 : j0 * 128 + 128] = block[
                        j0 * 16 : j0 * 16 + 16
                    ]
        return 0

    lax.fori_loop(0, 8, lines, 0)


def turn_left(ih, in_ref, rows_ref, left_ref):
    rows_ref[0:768, :] = in_ref[ih].reshape(768, 128).astype(F32)
    lane = lax.broadcasted_iota(jnp.int32, (8, 128), 1)
    highs = {bit: (lane // (16 * bit)) % 2 == 1 for bit in (1, 2, 4)}
    for tile in range(6):
        for il in range(2):
            blocks = []
            for q in range(tile * 8, tile * 8 + 8):
                at = (q // 3) * 48 + (q % 3) * 2 + il
                blocks.append(rows_ref[pl.ds(at, 8, stride=6), :])
            for bit in (1, 2, 4):
                turned = list(blocks)
                for n in range(8):
                    if n & bit:
                        continue
                    one, two = blocks[n], blocks[n + bit]
                    turned[n] = jnp.where(highs[bit], pltpu.roll(two, 16 * bit, 1), one)
                    turned[n + bit] = jnp.where(
                        highs[bit], two, pltpu.roll(one, 128 - 16 * bit, 1)
                    )
                blocks = turned
            for i0 in range(0, 8, 2):
                at = (il * 8 + i0) * 8
                left_ref[at : at + 16, tile * 128 : tile * 128 + 128] = jnp.concatenate(
                    blocks[i0 : i0 + 2], axis=0
                ).astype(BF16)


def multiply(ih, left_ref, right_ref, z_ref, rows_ref, msg_ref):
    for n in range(4):
        made = jnp.dot(
            left_ref[...], right_ref[:, n * 256 : n * 256 + 256], preferred_element_type=F32
        )
        made = made * 768**-0.5
        for e in range(2):
            for i16 in range(16):
                z_ref[pl.ds(i16 * 8 + n * 2 + e, 8, stride=136), :] = made[
                    i16 * 8 : i16 * 8 + 8, e * 128 : e * 128 + 128
                ]
    for ia in range(8):
        block = z_ref[ia * 136 : ia * 136 + 128, :].T
        for jb in range(16):
            at = (ia * 16 + jb) * 6
            rows_ref[at : at + 6, :] = block[jb * 8 : jb * 8 + 6]
    for n in range(4):
        rows = rows_ref[n * 192 : n * 192 + 192, :]
        msg_ref[ih, n * 96 : n * 96 + 96] = rows.astype(BF16).reshape(96, 2, 128)


def finish(ih, in_ref, column, w_ref, gate_ref, rows_ref, out_ref):
    rows_ref[0:768, :] = in_ref[ih].reshape(768, 128).astype(F32)
    i_at = pl.ds(ih * 16, 16)
    for jp in range(3):
        halves = []
        for e in range(2):
            mixed = rows_ref[pl.ds(jp * 2 + e, 128, stride=6), :]
            scaled = norm(mixed, column, 0).T.astype(BF16)
            made = jnp.dot(scaled, w_ref[...], preferred_element_type=F32)
            halves.append(made.reshape(16, 8, 128))
        made = jnp.concatenate(halves, axis=1) * gate_ref[i_at, jp * 16 : jp * 16 + 16, :]
        out_ref[i_at, jp * 16 : jp * 16 + 16, :] = made.astype(BF16)


def kernel(
    x_ref, in_gain_ref, wl_ref, wr_ref, mid_gain_ref, wo_ref, wg_ref, out_ref,
    ready_ref, gate_ref, rows_ref, rmsg_ref, lmsg_ref, rin_ref, lin_ref, pad_ref,
    right_ref, left_ref, z_ref, cmsg_ref, cin_ref, send, recv,
):
    a, b = lax.axis_index("first"), lax.axis_index("second")
    half, mine, core = a // 8, a * 8 + b // 2, lax.rem(b, 2)
    home = lax.rem(a, 8) * 16 + b
    own = half == core
    partner = a * 16 + b + 1 - 2 * core
    barrier = pltpu.get_barrier_semaphore()

    def greet(c):
        pl.semaphore_signal(barrier, inc=1, device_id=core * 128 + c, device_id_type=LOGICAL)

    def copy(src, dst, n, device):
        return pltpu.make_async_remote_copy(
            src_ref=src,
            dst_ref=dst,
            send_sem=send.at[n],
            recv_sem=recv.at[n],
            device_id=device,
            device_id_type=LOGICAL,
        )

    def spread(start, n, src, dst, device, keep):
        around(start, lambda c: copy(src(c), dst, n, device(c)).start())

        @pl.when(jnp.logical_not(own))
        def _():
            copy(src(start), dst, n, device(start)).start()

        @pl.when(own)
        def _():
            keep()

    def settle(ref, rows, sem):
        @pl.when(own)
        def _():
            view = ref.at[pl.ds(0, 127 * rows)]
            pltpu.make_async_copy(view, view, sem).wait()

        @pl.when(jnp.logical_not(own))
        def _():
            view = ref.at[pl.ds(0, 128 * rows)]
            pltpu.make_async_copy(view, view, sem).wait()

    around(home, greet)
    greet(home)
    pl.semaphore_signal(barrier, inc=1, device_id=partner, device_id_type=LOGICAL)
    make_right(x_ref, in_gain_ref, wr_ref, ready_ref, rows_ref, rmsg_ref)
    pl.semaphore_wait(barrier, 129)

    def keep_right():
        rin_ref[b, pl.ds(a * 9, 9)] = rmsg_ref[pl.ds(mine * 9, 9)]

    spread(
        mine,
        0,
        lambda c: rmsg_ref.at[pl.ds(c * 9, 9)],
        rin_ref.at[b, pl.ds(a * 9, 9)],
        lambda c: c * 2 + half,
        keep_right,
    )
    make_left(wl_ref, ready_ref, rows_ref, lmsg_ref)
    slot = b * 8 + lax.rem(a, 8)
    for ih in range(3):

        def keep_left():
            lin_ref[ih, pl.ds(slot * 3, 3)] = lmsg_ref[ih, pl.ds(mine * 3, 3)]

        spread(
            mine,
            1 + ih,
            lambda c: lmsg_ref.at[ih, pl.ds(c * 3, 3)],
            lin_ref.at[ih, pl.ds(slot * 3, 3)],
            lambda c: c * 2 + half,
            keep_left,
        )
    make_gate(wg_ref, ready_ref, gate_ref)
    settle(rmsg_ref, 9, recv.at[0])
    lines = rin_ref.at[:, pl.ds(core * 72, 72)]
    swap = copy(lines, lines, 7, partner)
    swap.start()
    swap.wait()
    turn_right(rin_ref, pad_ref, right_ref)
    for ih in range(3):
        settle(lmsg_ref.at[0], 3, recv.at[1 + ih])
        turn_left(ih, lin_ref, rows_ref, left_ref)
        multiply(ih, left_ref, right_ref, z_ref, rows_ref, cmsg_ref)

        def keep_product():
            cin_ref[ih, pl.ds(mine * 3, 3)] = cmsg_ref[ih, pl.ds(home * 3, 3)]

        spread(
            home,
            4 + ih,
            lambda c: cmsg_ref.at[ih, pl.ds(c * 3, 3)],
            cin_ref.at[ih, pl.ds(mine * 3, 3)],
            lambda c: core * 128 + c,
            keep_product,
        )
    column = jnp.broadcast_to(mid_gain_ref[...], (128, 128)).T
    for ih in range(3):
        settle(cmsg_ref.at[0], 3, recv.at[4 + ih])
        finish(ih, cin_ref, column, wo_ref, gate_ref, rows_ref, out_ref)
    settle(rmsg_ref, 9, send.at[0])
    for n in range(1, 7):
        settle(cmsg_ref.at[0], 3, send.at[n])


def per_device(pair_state, in_gain, left_weight, right_weight, mid_gain, out_weight, out_gate):
    return pl.pallas_call(
        kernel,
        name="triangle",
        out_shape=jax.ShapeDtypeStruct((48, 48, 128), BF16),
        in_specs=[VMEM] * 7,
        out_specs=VMEM,
        scratch_shapes=[
            pltpu.VMEM((18, 128, 128), BF16),
            pltpu.VMEM((48, 48, 128), F32),
            pltpu.VMEM((2304, 128), F32),
            pltpu.VMEM((1152, 2, 128), BF16),
            pltpu.VMEM((3, 384, 2, 128), BF16),
            pltpu.VMEM((16, 144, 2, 128), BF16),
            pltpu.VMEM((3, 384, 2, 128), BF16),
            pltpu.VMEM((2, 296, 128), F32),
            pltpu.VMEM((768, 1024), BF16),
            pltpu.VMEM((128, 768), BF16),
            pltpu.VMEM((8 * 136, 128), F32),
            pltpu.VMEM((3, 384, 2, 128), BF16),
            pltpu.VMEM((3, 384, 2, 128), BF16),
            pltpu.SemaphoreType.DMA((8,)),
            pltpu.SemaphoreType.DMA((8,)),
        ],
        compiler_params=pltpu.CompilerParams(collective_id=1, has_side_effects=True),
    )(
        pair_state,
        in_gain.reshape(1, 128),
        left_weight,
        right_weight,
        mid_gain.reshape(1, 128),
        out_weight,
        out_gate,
    )


def solution(mesh):
    in_specs = (P("first", "second", None), P(), P(), P(), P(), P(), P())
    out_specs = P("first", "second", None)
    return jax.shard_map(
        per_device, mesh=mesh, in_specs=in_specs, out_specs=out_specs, check_vma=False
    )
```

```python
import jax
import jax.numpy as jnp
from jax import lax
from jax.experimental import pallas as pl
from jax.experimental.pallas import tpu as pltpu
from jax.sharding import PartitionSpec as P

LOGICAL = pl.DeviceIdType.LOGICAL
F32, BF16 = jnp.float32, jnp.bfloat16
VMEM = pl.BlockSpec(memory_space=pltpu.VMEM)
NT = (((1,), (1,)), ((), ()))


def norm(values, gain, axis):
    centred = values - jnp.mean(values, axis=axis, keepdims=True)
    scale = lax.rsqrt(jnp.mean(centred * centred, axis=axis, keepdims=True) + 1e-05)
    return centred * scale * gain


FAR_FIRST = [(dy, dx) for dy in (2, 1, 3, 0) for dx in (2, 1, 3, 0)]


def ring(at, by, size):
    return jnp.where(at + by >= size, at + by - size, at + by)


def outward(z, lines, step, last):
    def plane(n, _):
        m = (n + 1) // 2
        there = ring(z, jnp.where(n % 2 == 0, 4 + m, 4 - m), 8)
        for line in lines:
            step(line, there)
        return 0

    lax.fori_loop(0, 7, plane, 0)
    for line in lines[:-1]:
        step(line, z)
    last()


def make_right(x_ref, gain_ref, w_ref, ready_ref, rows_ref, msg_ref):
    gain = gain_ref[...]
    weights = w_ref[...].astype(F32).T.astype(BF16)

    def tiles(k1, _):
        for i1 in range(6):
            block = x_ref[i1 * 8 : i1 * 8 + 8, pl.ds(pl.multiple_of(k1 * 16, 16), 16), :]
            ready = norm(block.astype(F32).reshape(128, 128), gain, 1).astype(BF16)
            ready_ref[k1 * 6 + i1] = ready
            made = lax.dot_general(weights, ready, NT, preferred_element_type=F32)
            rows_ref[pl.ds(k1 * 6 + i1, 128, stride=18), :] = made
        return 0

    lax.fori_loop(0, 3, tiles, 0)

    def pack(n, _):
        rows = rows_ref[pl.ds(pl.multiple_of(n * 288, 8), 288), :]
        msg_ref[pl.ds(n * 144, 144)] = rows.astype(BF16).reshape(144, 2, 128)
        return 0

    lax.fori_loop(0, 8, pack, 0)


def make_left(w_ref, ready_ref, rows_ref, msg_ref):
    weights = w_ref[...].astype(F32).T.astype(BF16)

    def tiles(k1, _):
        for i1 in range(6):
            made = lax.dot_general(
                weights, ready_ref[k1 * 6 + i1], NT, preferred_element_type=F32
            )
            at = (i1 // 2) * 768 + k1 * 2 + i1 % 2
            rows_ref[pl.ds(at, 128, stride=6), :] = made
        return 0

    lax.fori_loop(0, 3, tiles, 0)
    for ih in range(3):

        def pack(n, _):
            rows = rows_ref[pl.ds(pl.multiple_of(ih * 768 + n * 192, 8), 192), :]
            msg_ref[ih, pl.ds(n * 96, 96)] = rows.astype(BF16).reshape(96, 2, 128)
            return 0

        lax.fori_loop(0, 4, pack, 0)


def make_gate(w_ref, ready_ref, gate_ref):
    weights = w_ref[...]

    def tiles(k1, _):
        for i1 in range(6):
            made = jnp.dot(ready_ref[k1 * 6 + i1], weights, preferred_element_type=F32)
            gate = jax.nn.sigmoid(made).reshape(8, 16, 128)
            gate_ref[i1 * 8 : i1 * 8 + 8, pl.ds(pl.multiple_of(k1 * 16, 16), 16), :] = gate
        return 0

    lax.fori_loop(0, 3, tiles, 0)


def turn_right(in_ref, pad_ref, right_ref):
    def lines(n, _):
        for e in range(2):
            b = n * 2 + e
            pad_ref[e, 0:288, :] = in_ref[b].reshape(288, 128).astype(F32)
            for k1 in range(3):
                parts = [pad_ref[e, ja * 18 + k1 * 6 : ja * 18 + k1 * 6 + 8, :] for ja in range(16)]
                block = jnp.concatenate(parts, axis=0).T.astype(BF16)
                at = pl.multiple_of(b * 48 + k1 * 16, 16)
                for j0 in range(8):
                    right_ref[pl.ds(at, 16), j0 * 128 : j0 * 128 + 128] = block[
                        j0 * 16 : j0 * 16 + 16
                    ]
        return 0

    lax.fori_loop(0, 8, lines, 0)


def turn_left(ih, in_ref, rows_ref, left_ref):
    rows_ref[0:768, :] = in_ref[ih].reshape(768, 128).astype(F32)
    lane = lax.broadcasted_iota(jnp.int32, (8, 128), 1)
    highs = {bit: (lane // (16 * bit)) % 2 == 1 for bit in (1, 2, 4)}
    for tile in range(6):
        for il in range(2):
            blocks = []
            for q in range(tile * 8, tile * 8 + 8):
                at = (q // 3) * 48 + (q % 3) * 2 + il
                blocks.append(rows_ref[pl.ds(at, 8, stride=6), :])
            for bit in (1, 2, 4):
                turned = list(blocks)
                for n in range(8):
                    if n & bit:
                        continue
                    one, two = blocks[n], blocks[n + bit]
                    turned[n] = jnp.where(highs[bit], pltpu.roll(two, 16 * bit, 1), one)
                    turned[n + bit] = jnp.where(
                        highs[bit], two, pltpu.roll(one, 128 - 16 * bit, 1)
                    )
                blocks = turned
            for i0 in range(0, 8, 2):
                at = (il * 8 + i0) * 8
                left_ref[at : at + 16, tile * 128 : tile * 128 + 128] = jnp.concatenate(
                    blocks[i0 : i0 + 2], axis=0
                ).astype(BF16)


def multiply(ih, left_ref, right_ref, z_ref, rows_ref, msg_ref):
    for n in range(4):
        made = jnp.dot(
            left_ref[...], right_ref[:, n * 256 : n * 256 + 256], preferred_element_type=F32
        )
        made = made * 768**-0.5
        for e in range(2):
            for i16 in range(16):
                z_ref[pl.ds(i16 * 8 + n * 2 + e, 8, stride=136), :] = made[
                    i16 * 8 : i16 * 8 + 8, e * 128 : e * 128 + 128
                ]
    for ia in range(8):
        block = z_ref[ia * 136 : ia * 136 + 128, :].T
        for jb in range(16):
            at = (ia * 16 + jb) * 6
            rows_ref[at : at + 6, :] = block[jb * 8 : jb * 8 + 6]
    for n in range(4):
        rows = rows_ref[n * 192 : n * 192 + 192, :]
        msg_ref[ih, n * 96 : n * 96 + 96] = rows.astype(BF16).reshape(96, 2, 128)


def finish(ih, in_ref, column, w_ref, gate_ref, rows_ref, out_ref):
    rows_ref[0:768, :] = in_ref[ih].reshape(768, 128).astype(F32)
    i_at = pl.ds(ih * 16, 16)
    for jp in range(3):
        halves = []
        for e in range(2):
            mixed = rows_ref[pl.ds(jp * 2 + e, 128, stride=6), :]
            scaled = norm(mixed, column, 0).T.astype(BF16)
            made = jnp.dot(scaled, w_ref[...], preferred_element_type=F32)
            halves.append(made.reshape(16, 8, 128))
        made = jnp.concatenate(halves, axis=1) * gate_ref[i_at, jp * 16 : jp * 16 + 16, :]
        out_ref[i_at, jp * 16 : jp * 16 + 16, :] = made.astype(BF16)


def kernel(
    x_hbm, in_gain_hbm, wl_hbm, wr_hbm, mid_gain_hbm, wo_hbm, wg_hbm, out_ref,
    x_ref, in_gain_ref, wl_ref, wr_ref, mid_gain_ref, wo_ref, wg_ref,
    ready_ref, gate_ref, rows_ref, rmsg_ref, lmsg_ref, rin_ref, lin_ref, pad_ref,
    right_ref, left_ref, z_ref, cmsg_ref, cin_ref, load, send, recv,
):
    hbm = (x_hbm, in_gain_hbm, wr_hbm, wl_hbm, mid_gain_hbm, wo_hbm, wg_hbm)
    vmem = (x_ref, in_gain_ref, wr_ref, wl_ref, mid_gain_ref, wo_ref, wg_ref)
    loads = [pltpu.make_async_copy(s, d, load.at[n]) for n, (s, d) in enumerate(zip(hbm, vmem))]
    for one in loads:
        one.start()
    a, b = lax.axis_index("first"), lax.axis_index("second")
    y, x, z, core = a // 4, lax.rem(a, 4), b // 2, lax.rem(b, 2)
    half, mine = a // 8, a * 8 + z
    home = lax.rem(a, 8) * 16 + b
    own = half == core
    partner = a * 16 + b + 1 - 2 * core
    barrier = pltpu.get_barrier_semaphore()

    out_lines = [ring(y, dy, 4) * 4 + ring(x, dx, 4) for dy, dx in FAR_FIRST]
    near = lax.rem(y, 2)
    back_lines = [
        (ya * 4 + ring(x, dx, 4), c)
        for ya in (1 - near, near)
        for dx in (2, 1, 3, 0)
        for c in (1 - core, core)
    ]

    def greet(line, there):
        pl.semaphore_signal(
            barrier,
            inc=1,
            device_id=core * 128 + line[0] * 16 + there * 2 + line[1],
            device_id_type=LOGICAL,
        )

    def copy(src, dst, n, device):
        return pltpu.make_async_remote_copy(
            src_ref=src,
            dst_ref=dst,
            send_sem=send.at[n],
            recv_sem=recv.at[n],
            device_id=device,
            device_id_type=LOGICAL,
        )

    def spread(n, lines, index, device, src, dst, keep):
        def step(line, there):
            copy(src(index(line, there)), dst, n, device(line, there)).start()

        def last():
            @pl.when(jnp.logical_not(own))
            def _():
                step(lines[-1], z)

            @pl.when(own)
            def _():
                keep()

        outward(z, lines, step, last)

    def out_index(line, there):
        return line * 8 + there

    def out_device(line, there):
        return line * 16 + there * 2 + half

    def back_index(line, there):
        return line[0] * 16 + there * 2 + line[1]

    def back_device(line, there):
        return core * 128 + back_index(line, there)

    def settle(ref, rows, sem):
        @pl.when(own)
        def _():
            view = ref.at[pl.ds(0, 127 * rows)]
            pltpu.make_async_copy(view, view, sem).wait()

        @pl.when(jnp.logical_not(own))
        def _():
            view = ref.at[pl.ds(0, 128 * rows)]
            pltpu.make_async_copy(view, view, sem).wait()

    outward(z, back_lines, greet, lambda: greet(back_lines[-1], z))
    pl.semaphore_signal(barrier, inc=1, device_id=partner, device_id_type=LOGICAL)
    for one in loads[:3]:
        one.wait()
    make_right(x_ref, in_gain_ref, wr_ref, ready_ref, rows_ref, rmsg_ref)
    pl.semaphore_wait(barrier, 129)

    def keep_right():
        rin_ref[b, pl.ds(a * 9, 9)] = rmsg_ref[pl.ds(mine * 9, 9)]

    spread(
        0,
        out_lines,
        out_index,
        out_device,
        lambda c: rmsg_ref.at[pl.ds(c * 9, 9)],
        rin_ref.at[b, pl.ds(a * 9, 9)],
        keep_right,
    )
    for one in loads[3:]:
        one.wait()
    make_left(wl_ref, ready_ref, rows_ref, lmsg_ref)
    slot = b * 8 + lax.rem(a, 8)
    for ih in range(3):

        def keep_left():
            lin_ref[ih, pl.ds(slot * 3, 3)] = lmsg_ref[ih, pl.ds(mine * 3, 3)]

        spread(
            1 + ih,
            out_lines,
            out_index,
            out_device,
            lambda c: lmsg_ref.at[ih, pl.ds(c * 3, 3)],
            lin_ref.at[ih, pl.ds(slot * 3, 3)],
            keep_left,
        )
    make_gate(wg_ref, ready_ref, gate_ref)
    settle(rmsg_ref, 9, recv.at[0])
    lines = rin_ref.at[:, pl.ds(core * 72, 72)]
    swap = copy(lines, lines, 7, partner)
    swap.start()
    swap.wait()
    turn_right(rin_ref, pad_ref, right_ref)
    for ih in range(3):
        settle(lmsg_ref.at[0], 3, recv.at[1 + ih])
        turn_left(ih, lin_ref, rows_ref, left_ref)
        multiply(ih, left_ref, right_ref, z_ref, rows_ref, cmsg_ref)

        def keep_product():
            cin_ref[ih, pl.ds(mine * 3, 3)] = cmsg_ref[ih, pl.ds(home * 3, 3)]

        spread(
            4 + ih,
            back_lines,
            back_index,
            back_device,
            lambda c: cmsg_ref.at[ih, pl.ds(c * 3, 3)],
            cin_ref.at[ih, pl.ds(mine * 3, 3)],
            keep_product,
        )
    column = jnp.broadcast_to(mid_gain_ref[...], (128, 128)).T
    for ih in range(3):
        settle(cmsg_ref.at[0], 3, recv.at[4 + ih])
        finish(ih, cin_ref, column, wo_ref, gate_ref, rows_ref, out_ref)
    settle(rmsg_ref, 9, send.at[0])
    for n in range(1, 7):
        settle(cmsg_ref.at[0], 3, send.at[n])


def per_device(pair_state, in_gain, left_weight, right_weight, mid_gain, out_weight, out_gate):
    return pl.pallas_call(
        kernel,
        name="triangle",
        out_shape=pltpu.VMEM((48, 48, 128), BF16),
        in_specs=[pl.BlockSpec(memory_space=pl.ANY)] * 7,
        out_specs=VMEM,
        scratch_shapes=[
            pltpu.VMEM((48, 48, 128), BF16),
            pltpu.VMEM((1, 128), F32),
            pltpu.VMEM((128, 128), BF16),
            pltpu.VMEM((128, 128), BF16),
            pltpu.VMEM((1, 128), F32),
            pltpu.VMEM((128, 128), BF16),
            pltpu.VMEM((128, 128), BF16),
            pltpu.VMEM((18, 128, 128), BF16),
            pltpu.VMEM((48, 48, 128), F32),
            pltpu.VMEM((2304, 128), F32),
            pltpu.VMEM((1152, 2, 128), BF16),
            pltpu.VMEM((3, 384, 2, 128), BF16),
            pltpu.VMEM((16, 144, 2, 128), BF16),
            pltpu.VMEM((3, 384, 2, 128), BF16),
            pltpu.VMEM((2, 296, 128), F32),
            pltpu.VMEM((768, 1024), BF16),
            pltpu.VMEM((128, 768), BF16),
            pltpu.VMEM((8 * 136, 128), F32),
            pltpu.VMEM((3, 384, 2, 128), BF16),
            pltpu.VMEM((3, 384, 2, 128), BF16),
            pltpu.SemaphoreType.DMA((7,)),
            pltpu.SemaphoreType.DMA((8,)),
            pltpu.SemaphoreType.DMA((8,)),
        ],
        compiler_params=pltpu.CompilerParams(collective_id=1, has_side_effects=True),
    )(
        pair_state,
        in_gain.reshape(1, 128),
        left_weight,
        right_weight,
        mid_gain.reshape(1, 128),
        out_weight,
        out_gate,
    )


def solution(mesh):
    in_specs = (P("first", "second", None), P(), P(), P(), P(), P(), P())
    out_specs = P("first", "second", None)
    return jax.shard_map(
        per_device, mesh=mesh, in_specs=in_specs, out_specs=out_specs, check_vma=False
    )
```

```python
import jax
import jax.numpy as jnp
from jax import lax
from jax.experimental import pallas as pl
from jax.experimental.pallas import tpu as pltpu
from jax.sharding import PartitionSpec as P

LOGICAL = pl.DeviceIdType.LOGICAL
F32, BF16 = jnp.float32, jnp.bfloat16
VMEM = pl.BlockSpec(memory_space=pltpu.VMEM)
NT = (((1,), (1,)), ((), ()))


def norm(values, gain, axis):
    centred = values - jnp.mean(values, axis=axis, keepdims=True)
    scale = lax.rsqrt(jnp.mean(centred * centred, axis=axis, keepdims=True) + 1e-05)
    return centred * scale * gain


def ring(at, by, size):
    return jnp.where(at + by >= size, at + by - size, at + by)


def inward(n):
    return jnp.where(n == 0, 2, jnp.where(n == 1, 1, jnp.where(n == 2, 3, 0)))


def heights(z):
    return [ring(z, dz, 8) for dz in (4, 3, 5, 2, 6, 1, 7)] + [z]


def outward(z, line_of, step, last):
    there = heights(z)

    def line(n, _):
        for other in there:
            step(line_of(n), other)
        return 0

    lax.fori_loop(0, 15, line, 0)
    for other in there[:-1]:
        step(line_of(jnp.int32(15)), other)
    last(line_of(jnp.int32(15)), z)


def make_right(x_ref, gain_ref, w_ref, ready_ref, rows_ref):
    gain = gain_ref[...]
    weights = w_ref[...].astype(F32).T.astype(BF16)

    def tiles(k1, _):
        for i1 in range(6):
            block = x_ref[i1 * 8 : i1 * 8 + 8, pl.ds(pl.multiple_of(k1 * 16, 16), 16), :]
            ready = norm(block.astype(F32).reshape(128, 128), gain, 1).astype(BF16)
            ready_ref[k1 * 6 + i1] = ready
            made = lax.dot_general(weights, ready, NT, preferred_element_type=F32)
            rows_ref[pl.ds(k1 * 6 + i1, 128, stride=18), :] = made
        return 0

    lax.fori_loop(0, 3, tiles, 0)


def pack_right(rows_ref, msg_ref):
    def pack(n, _):
        rows = rows_ref[pl.ds(pl.multiple_of(n * 288, 8), 288), :]
        msg_ref[pl.ds(n * 144, 144)] = rows.astype(BF16).reshape(144, 2, 128)
        return 0

    lax.fori_loop(0, 8, pack, 0)


def make_left(w_ref, ready_ref, rows_ref, msg_ref):
    weights = w_ref[...].astype(F32).T.astype(BF16)

    def tiles(k1, _):
        for i1 in range(6):
            made = lax.dot_general(
                weights, ready_ref[k1 * 6 + i1], NT, preferred_element_type=F32
            )
            at = (i1 // 2) * 768 + k1 * 2 + i1 % 2
            rows_ref[pl.ds(at, 128, stride=6), :] = made
        return 0

    lax.fori_loop(0, 3, tiles, 0)
    for ih in range(3):

        def pack(n, _):
            rows = rows_ref[pl.ds(pl.multiple_of(ih * 768 + n * 192, 8), 192), :]
            msg_ref[ih, pl.ds(n * 96, 96)] = rows.astype(BF16).reshape(96, 2, 128)
            return 0

        lax.fori_loop(0, 4, pack, 0)


def make_gate(w_ref, ready_ref, gate_ref):
    weights = w_ref[...]

    def tiles(k1, _):
        for i1 in range(6):
            made = jnp.dot(ready_ref[k1 * 6 + i1], weights, preferred_element_type=F32)
            gate = jax.nn.sigmoid(made).reshape(8, 16, 128)
            gate_ref[i1 * 8 : i1 * 8 + 8, pl.ds(pl.multiple_of(k1 * 16, 16), 16), :] = gate
        return 0

    lax.fori_loop(0, 3, tiles, 0)


def turn_right(in_ref, pad_ref, right_ref):
    def lines(n, _):
        for e in range(2):
            b = n * 2 + e
            pad_ref[e, 0:288, :] = in_ref[b].reshape(288, 128).astype(F32)
            for k1 in range(3):
                parts = [pad_ref[e, ja * 18 + k1 * 6 : ja * 18 + k1 * 6 + 8, :] for ja in range(16)]
                block = jnp.concatenate(parts, axis=0).T.astype(BF16)
                at = pl.multiple_of(b * 48 + k1 * 16, 16)
                for j0 in range(8):
                    right_ref[pl.ds(at, 16), j0 * 128 : j0 * 128 + 128] = block[
                        j0 * 16 : j0 * 16 + 16
                    ]
        return 0

    lax.fori_loop(0, 8, lines, 0)


def turn_left(ih, in_ref, rows_ref, left_ref):
    rows_ref[0:768, :] = in_ref[ih].reshape(768, 128).astype(F32)
    lane = lax.broadcasted_iota(jnp.int32, (8, 128), 1)
    highs = {bit: (lane // (16 * bit)) % 2 == 1 for bit in (1, 2, 4)}
    for tile in range(6):
        for il in range(2):
            blocks = []
            for q in range(tile * 8, tile * 8 + 8):
                at = (q // 3) * 48 + (q % 3) * 2 + il
                blocks.append(rows_ref[pl.ds(at, 8, stride=6), :])
            for bit in (1, 2, 4):
                turned = list(blocks)
                for n in range(8):
                    if n & bit:
                        continue
                    one, two = blocks[n], blocks[n + bit]
                    turned[n] = jnp.where(highs[bit], pltpu.roll(two, 16 * bit, 1), one)
                    turned[n + bit] = jnp.where(
                        highs[bit], two, pltpu.roll(one, 128 - 16 * bit, 1)
                    )
                blocks = turned
            for i0 in range(0, 8, 2):
                at = (il * 8 + i0) * 8
                left_ref[at : at + 16, tile * 128 : tile * 128 + 128] = jnp.concatenate(
                    blocks[i0 : i0 + 2], axis=0
                ).astype(BF16)


def multiply(ih, left_ref, right_ref, z_ref, rows_ref, msg_ref):
    for n in range(4):
        made = jnp.dot(
            left_ref[...], right_ref[:, n * 256 : n * 256 + 256], preferred_element_type=F32
        )
        made = made * 768**-0.5
        for e in range(2):
            for i16 in range(16):
                z_ref[pl.ds(i16 * 8 + n * 2 + e, 8, stride=136), :] = made[
                    i16 * 8 : i16 * 8 + 8, e * 128 : e * 128 + 128
                ]
    for ia in range(8):
        block = z_ref[ia * 136 : ia * 136 + 128, :].T
        for jb in range(16):
            at = (ia * 16 + jb) * 6
            rows_ref[at : at + 6, :] = block[jb * 8 : jb * 8 + 6]
    for n in range(4):
        rows = rows_ref[n * 192 : n * 192 + 192, :]
        msg_ref[ih, n * 96 : n * 96 + 96] = rows.astype(BF16).reshape(96, 2, 128)


def finish(ih, in_ref, column, w_ref, gate_ref, rows_ref, out_ref):
    rows_ref[0:768, :] = in_ref[ih].reshape(768, 128).astype(F32)
    i_at = pl.ds(ih * 16, 16)
    for jp in range(3):
        halves = []
        for e in range(2):
            mixed = rows_ref[pl.ds(jp * 2 + e, 128, stride=6), :]
            scaled = norm(mixed, column, 0).T.astype(BF16)
            made = jnp.dot(scaled, w_ref[...], preferred_element_type=F32)
            halves.append(made.reshape(16, 8, 128))
        made = jnp.concatenate(halves, axis=1) * gate_ref[i_at, jp * 16 : jp * 16 + 16, :]
        out_ref[i_at, jp * 16 : jp * 16 + 16, :] = made.astype(BF16)


def kernel(
    x_hbm, in_gain_hbm, wl_hbm, wr_hbm, mid_gain_hbm, wo_hbm, wg_hbm, out_ref,
    x_ref, in_gain_ref, wl_ref, wr_ref, mid_gain_ref, wo_ref, wg_ref,
    ready_ref, gate_ref, rows_ref, rmsg_ref, lmsg_ref, rin_ref, lin_ref, pad_ref,
    right_ref, left_ref, z_ref, cmsg_ref, cin_ref, load, send, recv, ready_sem,
):
    hbm = (x_hbm, in_gain_hbm, wr_hbm, wl_hbm, mid_gain_hbm, wo_hbm, wg_hbm)
    vmem = (x_ref, in_gain_ref, wr_ref, wl_ref, mid_gain_ref, wo_ref, wg_ref)
    loads = [pltpu.make_async_copy(s, d, load.at[n]) for n, (s, d) in enumerate(zip(hbm, vmem))]
    for one in loads:
        one.start()
    a, b = lax.axis_index("first"), lax.axis_index("second")
    y, x, z, core = a // 4, lax.rem(a, 4), b // 2, lax.rem(b, 2)
    half, mine = a // 8, a * 8 + z
    home = lax.rem(a, 8) * 16 + b
    own = half == core
    partner = a * 16 + b + 1 - 2 * core
    barrier = pltpu.get_barrier_semaphore()

    def out_line(n):
        return ring(y, inward(n // 4), 4) * 4 + ring(x, inward(n % 4), 4)

    def back_line(n):
        near = lax.rem(y, 2)
        ya = jnp.where(n < 8, 1 - near, near)
        c = jnp.where(n % 2 == 0, 1 - core, core)
        return (ya * 4 + ring(x, inward((n // 2) % 4), 4)) * 16 + c

    def greet(n, _):
        for sem, device in ((barrier, a * 16 + ring(b, n, 16)), (barrier, ring(a, n, 16) * 16 + b)):
            pl.semaphore_signal(sem, inc=1, device_id=device, device_id_type=LOGICAL)
        return 0

    def line_ready(n, _):
        there = ring(a, n, 16) * 16 + b
        pl.semaphore_signal(ready_sem.at[a], inc=1, device_id=there, device_id_type=LOGICAL)
        return 0

    def copy(src, dst, n, device):
        return pltpu.make_async_remote_copy(
            src_ref=src,
            dst_ref=dst,
            send_sem=send.at[n],
            recv_sem=recv.at[n],
            device_id=device,
            device_id_type=LOGICAL,
        )

    def spread(n, line_of, index, device, src, dst, keep):
        def step(line, there):
            copy(src(index(line, there)), dst, n, device(line, there)).start()

        def last(line, there):
            @pl.when(jnp.logical_not(own))
            def _():
                step(line, there)

            @pl.when(own)
            def _():
                keep()

        outward(z, line_of, step, last)

    def out_index(line, there):
        return line * 8 + there

    def out_device(line, there):
        return line * 16 + there * 2 + half

    def back_index(line, there):
        return line + there * 2

    def back_device(line, there):
        return core * 128 + back_index(line, there)

    def settle(ref, rows, sem):
        @pl.when(own)
        def _():
            view = ref.at[pl.ds(0, 127 * rows)]
            pltpu.make_async_copy(view, view, sem).wait()

        @pl.when(jnp.logical_not(own))
        def _():
            view = ref.at[pl.ds(0, 128 * rows)]
            pltpu.make_async_copy(view, view, sem).wait()

    lax.fori_loop(1, 16, greet, 0)
    for one in loads[:3]:
        one.wait()
    make_right(x_ref, in_gain_ref, wr_ref, ready_ref, rows_ref)
    pl.semaphore_wait(barrier, 30)
    lax.fori_loop(1, 16, line_ready, 0)
    pack_right(rows_ref, rmsg_ref)

    def send_right(line, there):
        c = out_index(line, there)
        dst = rin_ref.at[b, pl.ds(a * 9, 9)]
        copy(rmsg_ref.at[pl.ds(c * 9, 9)], dst, 0, out_device(line, there)).start()

    there = heights(z)
    for other in there[:-1]:
        send_right(a, other)

    @pl.when(jnp.logical_not(own))
    def _():
        send_right(a, z)

    @pl.when(own)
    def _():
        rin_ref[b, pl.ds(a * 9, 9)] = rmsg_ref[pl.ds(mine * 9, 9)]

    def right_line(n, _):
        line = out_line(14 - n)
        pl.semaphore_wait(ready_sem.at[line], 1)
        for other in there:
            send_right(line, other)
        return 0

    lax.fori_loop(0, 15, right_line, 0)
    for one in loads[3:]:
        one.wait()
    make_left(wl_ref, ready_ref, rows_ref, lmsg_ref)
    slot = b * 8 + lax.rem(a, 8)
    for ih in range(3):

        def keep_left():
            lin_ref[ih, pl.ds(slot * 3, 3)] = lmsg_ref[ih, pl.ds(mine * 3, 3)]

        spread(
            1 + ih,
            out_line,
            out_index,
            out_device,
            lambda c: lmsg_ref.at[ih, pl.ds(c * 3, 3)],
            lin_ref.at[ih, pl.ds(slot * 3, 3)],
            keep_left,
        )
    make_gate(wg_ref, ready_ref, gate_ref)
    settle(rmsg_ref, 9, recv.at[0])
    lines = rin_ref.at[:, pl.ds(core * 72, 72)]
    swap = copy(lines, lines, 7, partner)
    swap.start()
    swap.wait()
    turn_right(rin_ref, pad_ref, right_ref)
    for ih in range(3):
        settle(lmsg_ref.at[0], 3, recv.at[1 + ih])
        turn_left(ih, lin_ref, rows_ref, left_ref)
        multiply(ih, left_ref, right_ref, z_ref, rows_ref, cmsg_ref)

        def keep_product():
            cin_ref[ih, pl.ds(mine * 3, 3)] = cmsg_ref[ih, pl.ds(home * 3, 3)]

        spread(
            4 + ih,
            back_line,
            back_index,
            back_device,
            lambda c: cmsg_ref.at[ih, pl.ds(c * 3, 3)],
            cin_ref.at[ih, pl.ds(mine * 3, 3)],
            keep_product,
        )
    column = jnp.broadcast_to(mid_gain_ref[...], (128, 128)).T
    for ih in range(3):
        settle(cmsg_ref.at[0], 3, recv.at[4 + ih])
        finish(ih, cin_ref, column, wo_ref, gate_ref, rows_ref, out_ref)
    settle(rmsg_ref, 9, send.at[0])
    for n in range(1, 7):
        settle(cmsg_ref.at[0], 3, send.at[n])


def per_device(pair_state, in_gain, left_weight, right_weight, mid_gain, out_weight, out_gate):
    return pl.pallas_call(
        kernel,
        name="triangle",
        out_shape=pltpu.VMEM((48, 48, 128), BF16),
        in_specs=[pl.BlockSpec(memory_space=pl.ANY)] * 7,
        out_specs=VMEM,
        scratch_shapes=[
            pltpu.VMEM((48, 48, 128), BF16),
            pltpu.VMEM((1, 128), F32),
            pltpu.VMEM((128, 128), BF16),
            pltpu.VMEM((128, 128), BF16),
            pltpu.VMEM((1, 128), F32),
            pltpu.VMEM((128, 128), BF16),
            pltpu.VMEM((128, 128), BF16),
            pltpu.VMEM((18, 128, 128), BF16),
            pltpu.VMEM((48, 48, 128), F32),
            pltpu.VMEM((2304, 128), F32),
            pltpu.VMEM((1152, 2, 128), BF16),
            pltpu.VMEM((3, 384, 2, 128), BF16),
            pltpu.VMEM((16, 144, 2, 128), BF16),
            pltpu.VMEM((3, 384, 2, 128), BF16),
            pltpu.VMEM((2, 296, 128), F32),
            pltpu.VMEM((768, 1024), BF16),
            pltpu.VMEM((128, 768), BF16),
            pltpu.VMEM((8 * 136, 128), F32),
            pltpu.VMEM((3, 384, 2, 128), BF16),
            pltpu.VMEM((3, 384, 2, 128), BF16),
            pltpu.SemaphoreType.DMA((7,)),
            pltpu.SemaphoreType.DMA((8,)),
            pltpu.SemaphoreType.DMA((8,)),
            pltpu.SemaphoreType.REGULAR((16,)),
        ],
        compiler_params=pltpu.CompilerParams(collective_id=1, has_side_effects=True),
    )(
        pair_state,
        in_gain.reshape(1, 128),
        left_weight,
        right_weight,
        mid_gain.reshape(1, 128),
        out_weight,
        out_gate,
    )


def solution(mesh):
    in_specs = (P("first", "second", None), P(), P(), P(), P(), P(), P())
    out_specs = P("first", "second", None)
    return jax.shard_map(
        per_device, mesh=mesh, in_specs=in_specs, out_specs=out_specs, check_vma=False
    )
```

```python
import jax
import jax.numpy as jnp
from jax import lax
from jax.experimental import pallas as pl
from jax.experimental.pallas import tpu as pltpu
from jax.sharding import PartitionSpec as P

LOGICAL = pl.DeviceIdType.LOGICAL
F32, BF16 = jnp.float32, jnp.bfloat16
VMEM = pl.BlockSpec(memory_space=pltpu.VMEM)
NT = (((1,), (1,)), ((), ()))


def norm(values, gain, axis):
    centred = values - jnp.mean(values, axis=axis, keepdims=True)
    scale = lax.rsqrt(jnp.mean(centred * centred, axis=axis, keepdims=True) + 1e-05)
    return centred * scale * gain


def ring(at, by, size):
    return jnp.where(at + by >= size, at + by - size, at + by)


def inward(n):
    return jnp.where(n == 0, 2, jnp.where(n == 1, 1, jnp.where(n == 2, 3, 0)))


def heights(z):
    return [ring(z, dz, 8) for dz in (4, 3, 5, 2, 6, 1, 7)] + [z]


def outward(z, line_of, step, last):
    there = heights(z)

    def line(n, _):
        for other in there:
            step(line_of(n), other)
        return 0

    lax.fori_loop(0, 15, line, 0)
    for other in there[:-1]:
        step(line_of(jnp.int32(15)), other)
    last(line_of(jnp.int32(15)), z)


def make_right(part, x_ref, gain_ref, w_ref, ready_ref, rows_ref):
    gain = gain_ref[...]
    weights = w_ref[...].astype(F32).T.astype(BF16)

    def tiles(k1, _):
        part(k1).wait()
        for i1 in range(6):
            block = x_ref[i1 * 8 : i1 * 8 + 8, pl.ds(pl.multiple_of(k1 * 16, 16), 16), :]
            ready = norm(block.astype(F32).reshape(128, 128), gain, 1).astype(BF16)
            ready_ref[k1 * 6 + i1] = ready
            made = lax.dot_general(weights, ready, NT, preferred_element_type=F32)
            rows_ref[pl.ds(k1 * 6 + i1, 128, stride=18), :] = made
        return 0

    lax.fori_loop(0, 3, tiles, 0)


def pack_right(line, rows_ref, msg_ref):
    rows = rows_ref[pl.ds(pl.multiple_of(line * 144, 8), 144), :]
    msg_ref[pl.ds(line * 72, 72)] = rows.astype(BF16).reshape(72, 2, 128)


def make_left(w_ref, ready_ref, rows_ref, msg_ref):
    weights = w_ref[...].astype(F32).T.astype(BF16)

    def tiles(k1, _):
        for i1 in range(6):
            made = lax.dot_general(
                weights, ready_ref[k1 * 6 + i1], NT, preferred_element_type=F32
            )
            at = (i1 // 2) * 768 + k1 * 2 + i1 % 2
            rows_ref[pl.ds(at, 128, stride=6), :] = made
        return 0

    lax.fori_loop(0, 3, tiles, 0)
    for ih in range(3):

        def pack(n, _):
            rows = rows_ref[pl.ds(pl.multiple_of(ih * 768 + n * 192, 8), 192), :]
            msg_ref[ih, pl.ds(n * 96, 96)] = rows.astype(BF16).reshape(96, 2, 128)
            return 0

        lax.fori_loop(0, 4, pack, 0)


def make_gate(w_ref, ready_ref, gate_ref):
    weights = w_ref[...]

    def tiles(k1, _):
        for i1 in range(6):
            made = jnp.dot(ready_ref[k1 * 6 + i1], weights, preferred_element_type=F32)
            gate = jax.nn.sigmoid(made).reshape(8, 16, 128)
            gate_ref[i1 * 8 : i1 * 8 + 8, pl.ds(pl.multiple_of(k1 * 16, 16), 16), :] = gate
        return 0

    lax.fori_loop(0, 3, tiles, 0)


def turn_right(in_ref, pad_ref, right_ref):
    def lines(n, _):
        for e in range(2):
            b = n * 2 + e
            pad_ref[e, 0:288, :] = in_ref[b].reshape(288, 128).astype(F32)
            for k1 in range(3):
                parts = [pad_ref[e, ja * 18 + k1 * 6 : ja * 18 + k1 * 6 + 8, :] for ja in range(16)]
                block = jnp.concatenate(parts, axis=0).T.astype(BF16)
                at = pl.multiple_of(b * 48 + k1 * 16, 16)
                for j0 in range(8):
                    right_ref[pl.ds(at, 16), j0 * 128 : j0 * 128 + 128] = block[
                        j0 * 16 : j0 * 16 + 16
                    ]
        return 0

    lax.fori_loop(0, 8, lines, 0)


def turn_left(ih, in_ref, rows_ref, left_ref):
    rows_ref[0:768, :] = in_ref[ih].reshape(768, 128).astype(F32)
    lane = lax.broadcasted_iota(jnp.int32, (8, 128), 1)
    highs = {bit: (lane // (16 * bit)) % 2 == 1 for bit in (1, 2, 4)}
    for tile in range(6):
        for il in range(2):
            blocks = []
            for q in range(tile * 8, tile * 8 + 8):
                at = (q // 3) * 48 + (q % 3) * 2 + il
                blocks.append(rows_ref[pl.ds(at, 8, stride=6), :])
            for bit in (1, 2, 4):
                turned = list(blocks)
                for n in range(8):
                    if n & bit:
                        continue
                    one, two = blocks[n], blocks[n + bit]
                    turned[n] = jnp.where(highs[bit], pltpu.roll(two, 16 * bit, 1), one)
                    turned[n + bit] = jnp.where(
                        highs[bit], two, pltpu.roll(one, 128 - 16 * bit, 1)
                    )
                blocks = turned
            for i0 in range(0, 8, 2):
                at = (il * 8 + i0) * 8
                left_ref[at : at + 16, tile * 128 : tile * 128 + 128] = jnp.concatenate(
                    blocks[i0 : i0 + 2], axis=0
                ).astype(BF16)


def multiply(ih, left_ref, right_ref, z_ref, rows_ref, msg_ref):
    for n in range(4):
        made = jnp.dot(
            left_ref[...], right_ref[:, n * 256 : n * 256 + 256], preferred_element_type=F32
        )
        made = made * 768**-0.5
        for e in range(2):
            for i16 in range(16):
                z_ref[pl.ds(i16 * 8 + n * 2 + e, 8, stride=136), :] = made[
                    i16 * 8 : i16 * 8 + 8, e * 128 : e * 128 + 128
                ]
    for ia in range(8):
        block = z_ref[ia * 136 : ia * 136 + 128, :].T
        for jb in range(16):
            at = (ia * 16 + jb) * 6
            rows_ref[at : at + 6, :] = block[jb * 8 : jb * 8 + 6]
    for n in range(4):
        rows = rows_ref[n * 192 : n * 192 + 192, :]
        msg_ref[ih, n * 96 : n * 96 + 96] = rows.astype(BF16).reshape(96, 2, 128)


def finish(ih, in_ref, column, w_ref, gate_ref, rows_ref, out_ref):
    rows_ref[0:768, :] = in_ref[ih].reshape(768, 128).astype(F32)
    i_at = pl.ds(ih * 16, 16)
    for jp in range(3):
        halves = []
        for e in range(2):
            mixed = rows_ref[pl.ds(jp * 2 + e, 128, stride=6), :]
            scaled = norm(mixed, column, 0).T.astype(BF16)
            made = jnp.dot(scaled, w_ref[...], preferred_element_type=F32)
            halves.append(made.reshape(16, 8, 128))
        made = jnp.concatenate(halves, axis=1) * gate_ref[i_at, jp * 16 : jp * 16 + 16, :]
        out_ref[i_at, jp * 16 : jp * 16 + 16, :] = made.astype(BF16)


def kernel(
    x_hbm, in_gain_hbm, wl_hbm, wr_hbm, mid_gain_hbm, wo_hbm, wg_hbm, out_ref,
    x_ref, in_gain_ref, wl_ref, wr_ref, mid_gain_ref, wo_ref, wg_ref,
    ready_ref, gate_ref, rows_ref, rmsg_ref, lmsg_ref, rin_ref, lin_ref, pad_ref,
    right_ref, left_ref, z_ref, cmsg_ref, cin_ref, load, send, recv, ready_sem,
):
    def part(k1):
        at = pl.ds(pl.multiple_of(k1 * 16, 16), 16)
        return pltpu.make_async_copy(x_hbm.at[:, at, :], x_ref.at[:, at, :], load.at[6 + k1])

    for k1 in range(3):
        part(k1).start()
    hbm = (in_gain_hbm, wr_hbm, wl_hbm, mid_gain_hbm, wo_hbm, wg_hbm)
    vmem = (in_gain_ref, wr_ref, wl_ref, mid_gain_ref, wo_ref, wg_ref)
    loads = [pltpu.make_async_copy(s, d, load.at[n]) for n, (s, d) in enumerate(zip(hbm, vmem))]
    for one in loads:
        one.start()
    a, b = lax.axis_index("first"), lax.axis_index("second")
    y, x, z, core = a // 4, lax.rem(a, 4), b // 2, lax.rem(b, 2)
    half, mine = a // 8, a * 8 + z
    home = lax.rem(a, 8) * 16 + b
    own = half == core
    partner = a * 16 + b + 1 - 2 * core
    barrier = pltpu.get_barrier_semaphore()

    def out_line(n):
        return ring(y, inward(n // 4), 4) * 4 + ring(x, inward(n % 4), 4)

    def back_line(n):
        near = lax.rem(y, 2)
        ya = jnp.where(n < 8, 1 - near, near)
        c = jnp.where(n % 2 == 0, 1 - core, core)
        return (ya * 4 + ring(x, inward((n // 2) % 4), 4)) * 16 + c

    def greet(n, _):
        for sem, device in ((barrier, a * 16 + ring(b, n, 16)), (barrier, ring(a, n, 16) * 16 + b)):
            pl.semaphore_signal(sem, inc=1, device_id=device, device_id_type=LOGICAL)
        return 0

    def line_ready(n, _):
        there = ring(a, n, 16) * 16 + b
        pl.semaphore_signal(ready_sem.at[a], inc=1, device_id=there, device_id_type=LOGICAL)
        return 0

    def copy(src, dst, n, device):
        return pltpu.make_async_remote_copy(
            src_ref=src,
            dst_ref=dst,
            send_sem=send.at[n],
            recv_sem=recv.at[n],
            device_id=device,
            device_id_type=LOGICAL,
        )

    def spread(n, line_of, index, device, src, dst, keep):
        def step(line, there):
            copy(src(index(line, there)), dst, n, device(line, there)).start()

        def last(line, there):
            @pl.when(jnp.logical_not(own))
            def _():
                step(line, there)

            @pl.when(own)
            def _():
                keep()

        outward(z, line_of, step, last)

    def out_index(line, there):
        return line * 8 + there

    def out_device(line, there):
        return line * 16 + there * 2 + half

    def back_index(line, there):
        return line + there * 2

    def back_device(line, there):
        return core * 128 + back_index(line, there)

    def settle(ref, rows, sem):
        @pl.when(own)
        def _():
            view = ref.at[pl.ds(0, 127 * rows)]
            pltpu.make_async_copy(view, view, sem).wait()

        @pl.when(jnp.logical_not(own))
        def _():
            view = ref.at[pl.ds(0, 128 * rows)]
            pltpu.make_async_copy(view, view, sem).wait()

    lax.fori_loop(1, 16, greet, 0)
    for one in loads[:2]:
        one.wait()
    make_right(part, x_ref, in_gain_ref, wr_ref, ready_ref, rows_ref)
    pl.semaphore_wait(barrier, 30)
    lax.fori_loop(1, 16, line_ready, 0)

    def send_right(line, there):
        c = out_index(line, there)
        dst = rin_ref.at[b, pl.ds(a * 9, 9)]
        copy(rmsg_ref.at[pl.ds(c * 9, 9)], dst, 0, out_device(line, there)).start()

    there = heights(z)
    pack_right(a, rows_ref, rmsg_ref)
    pack_right(out_line(jnp.int32(14)), rows_ref, rmsg_ref)
    for other in there[:-1]:
        send_right(a, other)

    @pl.when(jnp.logical_not(own))
    def _():
        send_right(a, z)

    @pl.when(own)
    def _():
        rin_ref[b, pl.ds(a * 9, 9)] = rmsg_ref[pl.ds(mine * 9, 9)]

    def right_line(n, _):
        pack_right(out_line(13 - n), rows_ref, rmsg_ref)
        line = out_line(14 - n)
        pl.semaphore_wait(ready_sem.at[line], 1)
        for other in there:
            send_right(line, other)
        return 0

    lax.fori_loop(0, 14, right_line, 0)
    line = out_line(jnp.int32(0))
    pl.semaphore_wait(ready_sem.at[line], 1)
    for other in there:
        send_right(line, other)
    for one in loads[2:]:
        one.wait()
    make_left(wl_ref, ready_ref, rows_ref, lmsg_ref)
    slot = b * 8 + lax.rem(a, 8)
    for ih in range(3):

        def keep_left():
            lin_ref[ih, pl.ds(slot * 3, 3)] = lmsg_ref[ih, pl.ds(mine * 3, 3)]

        spread(
            1 + ih,
            out_line,
            out_index,
            out_device,
            lambda c: lmsg_ref.at[ih, pl.ds(c * 3, 3)],
            lin_ref.at[ih, pl.ds(slot * 3, 3)],
            keep_left,
        )
    make_gate(wg_ref, ready_ref, gate_ref)
    settle(rmsg_ref, 9, recv.at[0])
    lines = rin_ref.at[:, pl.ds(core * 72, 72)]
    swap = copy(lines, lines, 7, partner)
    swap.start()
    swap.wait()
    turn_right(rin_ref, pad_ref, right_ref)
    for ih in range(3):
        settle(lmsg_ref.at[0], 3, recv.at[1 + ih])
        turn_left(ih, lin_ref, rows_ref, left_ref)
        multiply(ih, left_ref, right_ref, z_ref, rows_ref, cmsg_ref)

        def keep_product():
            cin_ref[ih, pl.ds(mine * 3, 3)] = cmsg_ref[ih, pl.ds(home * 3, 3)]

        spread(
            4 + ih,
            back_line,
            back_index,
            back_device,
            lambda c: cmsg_ref.at[ih, pl.ds(c * 3, 3)],
            cin_ref.at[ih, pl.ds(mine * 3, 3)],
            keep_product,
        )
    column = jnp.broadcast_to(mid_gain_ref[...], (128, 128)).T
    for ih in range(3):
        settle(cmsg_ref.at[0], 3, recv.at[4 + ih])
        finish(ih, cin_ref, column, wo_ref, gate_ref, rows_ref, out_ref)
    settle(rmsg_ref, 9, send.at[0])
    for n in range(1, 7):
        settle(cmsg_ref.at[0], 3, send.at[n])


def per_device(pair_state, in_gain, left_weight, right_weight, mid_gain, out_weight, out_gate):
    return pl.pallas_call(
        kernel,
        name="triangle",
        out_shape=pltpu.VMEM((48, 48, 128), BF16),
        in_specs=[pl.BlockSpec(memory_space=pl.ANY)] * 7,
        out_specs=VMEM,
        scratch_shapes=[
            pltpu.VMEM((48, 48, 128), BF16),
            pltpu.VMEM((1, 128), F32),
            pltpu.VMEM((128, 128), BF16),
            pltpu.VMEM((128, 128), BF16),
            pltpu.VMEM((1, 128), F32),
            pltpu.VMEM((128, 128), BF16),
            pltpu.VMEM((128, 128), BF16),
            pltpu.VMEM((18, 128, 128), BF16),
            pltpu.VMEM((48, 48, 128), F32),
            pltpu.VMEM((2304, 128), F32),
            pltpu.VMEM((1152, 2, 128), BF16),
            pltpu.VMEM((3, 384, 2, 128), BF16),
            pltpu.VMEM((16, 144, 2, 128), BF16),
            pltpu.VMEM((3, 384, 2, 128), BF16),
            pltpu.VMEM((2, 296, 128), F32),
            pltpu.VMEM((768, 1024), BF16),
            pltpu.VMEM((128, 768), BF16),
            pltpu.VMEM((8 * 136, 128), F32),
            pltpu.VMEM((3, 384, 2, 128), BF16),
            pltpu.VMEM((3, 384, 2, 128), BF16),
            pltpu.SemaphoreType.DMA((9,)),
            pltpu.SemaphoreType.DMA((8,)),
            pltpu.SemaphoreType.DMA((8,)),
            pltpu.SemaphoreType.REGULAR((16,)),
        ],
        compiler_params=pltpu.CompilerParams(collective_id=1, has_side_effects=True),
    )(
        pair_state,
        in_gain.reshape(1, 128),
        left_weight,
        right_weight,
        mid_gain.reshape(1, 128),
        out_weight,
        out_gate,
    )


def solution(mesh):
    in_specs = (P("first", "second", None), P(), P(), P(), P(), P(), P())
    out_specs = P("first", "second", None)
    return jax.shard_map(
        per_device, mesh=mesh, in_specs=in_specs, out_specs=out_specs, check_vma=False
    )
```
